512 devices in a mesh: gx: 4 (over x_lo, core), gy: 8 (over y), gz: 16 (over x_hi, z).
Axes of the slice: x: 4 (x_hi: 2, x_lo: 2; x = x_hi * 2 + x_lo), y: 8, z: 8, core: 2. Of those that a mesh axis runs over, the one named last changes fastest.
Arguments:
- features: bfloat16 [4, 8, 16, 16, 3200], P('gx', 'gy', 'gz'), may hold values from -6 to 6
- box_atoms: int32 [4, 8, 16], P('gx', 'gy', 'gz'), may hold values from 5 to 16, as said below
- edge_count: int32 [4, 8, 16], P('gx', 'gy', 'gz'), may hold values from 85 to 256, as said below
- edge_tower: int32 [4, 8, 16, 256], P('gx', 'gy', 'gz'), may hold values from 0 to 47, as said below
- edge_plate: int32 [4, 8, 16, 256], P('gx', 'gy', 'gz'), may hold values from 0 to 143, as said below
- wigner: float32 [4, 8, 16, 115, 256], P('gx', 'gy', 'gz'), may hold values from -1 to 1, as said below
- radial: bfloat16 [4, 8, 16, 256, 128], P('gx', 'gy', 'gz'), may hold values from 0.049804688 to 0.5
- so2_zero: bfloat16 [640, 640], replicated, may hold values from -0.25 to 0.25
- so2_one: bfloat16 [2, 512, 512], replicated, may hold values from -0.1875 to 0.1875
- so2_two: bfloat16 [2, 384, 384], replicated, may hold values from -0.21875 to 0.21875
Outputs:
- updated: bfloat16 [4, 8, 16, 16, 3200], P('gx', 'gy', 'gz')
The draws below stay inside these ranges and needn't reach their ends.
Inputs may be any that keep to these rules, and one draw needn't show every extreme that they name: `box_atoms`: the fullest box holds exactly 16 atoms in every draw; counts span a factor of three. `edge_count`: some device holds exactly 256 live edges in every draw. `edge_tower`: every entry d * 16 + a names an atom a present in tower box d, in live and padded slots alike. `edge_plate`: every entry p * 16 + a names an atom a present in plate box p, in live and padded slots alike. `wigner`: for each edge and degree, the rows are rows of an orthogonal matrix.
All inputs are finite; a program needn't handle non-finite values.
Results may differ from the reference program's by a relative error of at most 0.007.
Values may be sent and summed in bfloat16 or wider, within the bound.
A program may use at most 64 MiB of HBM per device.

```python
import math
import jax
import jax.numpy as jnp
from jax import lax

C = 128
DEGREE = 4
ORDER = 2
COEFS = 25
ATOMS = 16
EDGES = 256
BX = 4
BY = 8
BZ = 16


def atom_counts(key):
    lowest = max(1, ATOMS // 3)
    counts = jax.random.randint(jax.random.fold_in(key, 11), (BX, BY, BZ), lowest, ATOMS + 1)
    chosen = jax.random.randint(jax.random.fold_in(key, 12), (), 0, BX * BY * BZ)
    places = jnp.arange(BX * BY * BZ, dtype=jnp.int32).reshape(BX, BY, BZ)
    return jnp.where(places == chosen, ATOMS, counts).astype(jnp.int32)


def draw_box_atoms(key, part):
    return atom_counts(key)


def draw_edge_count(key, part):
    lowest = max(1, EDGES // 3)
    counts = jax.random.randint(jax.random.fold_in(key, 21), (BX, BY, BZ), lowest, EDGES + 1)
    chosen = jax.random.randint(jax.random.fold_in(key, 22), (), 0, BX * BY * BZ)
    places = jnp.arange(BX * BY * BZ, dtype=jnp.int32).reshape(BX, BY, BZ)
    return jnp.where(places == chosen, EDGES, counts).astype(jnp.int32)


def pick_atoms(key, neighbour_counts):
    slots = neighbour_counts.shape[0]
    which = jax.random.randint(jax.random.fold_in(key, 1), (BX, BY, BZ, EDGES), 0, slots)
    available = jnp.take_along_axis(jnp.moveaxis(neighbour_counts, 0, -1), which, axis=3)
    raw_bits = jax.random.randint(jax.random.fold_in(key, 2), (BX, BY, BZ, EDGES), 0, 1 << 20)
    return (which * ATOMS + raw_bits % available).astype(jnp.int32)


def draw_edge_tower(key, part):
    counts = atom_counts(key)
    beside_all = jnp.stack([jnp.roll(counts, -step_x, axis=0) for step_x in (-1, 0, 1)])
    return pick_atoms(jax.random.fold_in(key, 31), beside_all)


def draw_edge_plate(key, part):
    counts = atom_counts(key)
    beside_all = jnp.stack([jnp.roll(jnp.roll(counts, -step_y, axis=1), -step_z, axis=2) for step_y in (-1, 0, 1) for step_z in (-1, 0, 1)])
    return pick_atoms(jax.random.fold_in(key, 41), beside_all)


def draw_wigner(key, part):
    blocks = []
    for degree in range(DEGREE + 1):
        span_cols = 2 * degree + 1
        within = min(degree, ORDER)
        inner = jax.random.fold_in(key, 51 + degree)
        raw = jax.random.normal(inner, (BX, BY, BZ, EDGES, span_cols, span_cols), jnp.float32)
        raw = raw + 0.1 * jnp.eye(span_cols, dtype=jnp.float32)
        basis = jnp.linalg.qr(raw)[0]
        kept = basis[..., degree - within:degree + within + 1, :]
        kept = kept.reshape(BX, BY, BZ, EDGES, (2 * within + 1) * span_cols)
        blocks.append(jnp.moveaxis(kept, 3, 4))
    return jnp.concatenate(blocks, axis=3).astype(jnp.float32)


def block_levels(stream_key, extent, split, smallest, largest):
    loudness = 1.0
    for axis_at, shards_of in split:
        heights = jax.random.uniform(jax.random.fold_in(jax.random.fold_in(stream_key, 6), axis_at), (shards_of,), jnp.float32, smallest / len(split), largest / len(split))
        loudness = loudness * jnp.repeat(jnp.exp(heights), extent[axis_at] // shards_of).reshape((-1,) + (1,) * (len(extent) - 1 - axis_at))
    return loudness


def bell_draw(rng, extent, scale, most, cuts=(), kind=jnp.bfloat16):
    factor_of = block_levels(rng, extent, cuts, -0.22, 0.18) if cuts else 1.0
    drawn = jax.random.normal(rng, extent, jnp.float32) * scale * factor_of
    return jnp.minimum(jnp.maximum(drawn, -most), most).astype(kind)


def setup_inputs(seed: int = 0) -> dict:
    seeds = jax.random.split(jax.random.key(seed), 11)
    return {
        "features": bell_draw(seeds[0], (BX, BY, BZ, ATOMS, COEFS * C), 1.0, 6.0, ((0, 4), (1, 8), (2, 16))),
        "box_atoms": draw_box_atoms(jax.random.fold_in(seeds[10], 71), 0),
        "edge_count": draw_edge_count(jax.random.fold_in(seeds[10], 71), 0),
        "edge_tower": draw_edge_tower(jax.random.fold_in(seeds[10], 71), 0),
        "edge_plate": draw_edge_plate(jax.random.fold_in(seeds[10], 71), 0),
        "wigner": draw_wigner(jax.random.fold_in(seeds[10], 71), 0),
        "radial": jnp.clip(jnp.exp(math.log(0.5) - 2.306499 * jax.random.uniform(seeds[6], (BX, BY, BZ, EDGES, C), jnp.float32) ** block_levels(seeds[6], (BX, BY, BZ, EDGES, C), ((0, 4), (1, 8), (2, 16)), -0.2, 0.2)), 0.049804688, 0.5).astype(jnp.bfloat16),
        "so2_zero": bell_draw(seeds[7], ((DEGREE + 1) * C, (DEGREE + 1) * C), ((DEGREE + 1) * C) ** -0.5, 0.25),
        "so2_one": bell_draw(seeds[8], (2, DEGREE * C, DEGREE * C), (2 * DEGREE * C) ** -0.5, 0.1875),
        "so2_two": bell_draw(seeds[9], (2, (DEGREE - 1) * C, (DEGREE - 1) * C), (2 * (DEGREE - 1) * C) ** -0.5, 0.21875),
    }


def rotate_forward(edge_rows, wig):
    pieces = {}
    offset = 0
    for degree in range(DEGREE + 1):
        within = min(degree, ORDER)
        for azimuth in range(-within, within + 1):
            summed = jnp.zeros((edge_rows.shape[0], edge_rows.shape[2]), jnp.float32)
            for column in range(-degree, degree + 1):
                summed = summed + wig[offset][:, None] * edge_rows[:, degree * degree + degree + column, :]
                offset += 1
            pieces[degree, azimuth] = summed
    return pieces

def rotate_back(pieces, wig):
    blocks = []
    offset = 0
    for degree in range(DEGREE + 1):
        within = min(degree, ORDER)
        span_cols = 2 * degree + 1
        summed = [None] * span_cols
        for azimuth in range(-within, within + 1):
            for column in range(span_cols):
                product = wig[offset][:, None] * pieces[degree, azimuth]
                summed[column] = product if summed[column] is None else summed[column] + product
                offset += 1
        blocks.extend(summed)
    return jnp.stack(blocks, axis=1)

def mix_orders(pieces, gate, so2_zero, so2_one, so2_two):
    channels = gate.shape[1]

    def lowered(degree, azimuth):
        return (pieces[degree, azimuth] * gate).astype(jnp.bfloat16)
    result = {}
    zeroth = jnp.concatenate([lowered(degree, 0) for degree in range(DEGREE + 1)], axis=1)
    mixed = jnp.dot(zeroth.astype(jnp.float32), so2_zero.astype(jnp.float32), preferred_element_type=jnp.float32)
    for degree in range(DEGREE + 1):
        result[degree, 0] = mixed[:, degree * channels:(degree + 1) * channels]
    for azimuth, table in ((1, so2_one), (2, so2_two)):
        degrees = list(range(azimuth, DEGREE + 1))
        plus = jnp.concatenate([lowered(degree, azimuth) for degree in degrees], axis=1)
        minus = jnp.concatenate([lowered(degree, -azimuth) for degree in degrees], axis=1)
        real_part = jnp.dot(plus.astype(jnp.float32), table[0].astype(jnp.float32), preferred_element_type=jnp.float32) - jnp.dot(minus.astype(jnp.float32), table[1].astype(jnp.float32), preferred_element_type=jnp.float32)
        imag_part = jnp.dot(plus.astype(jnp.float32), table[1].astype(jnp.float32), preferred_element_type=jnp.float32) + jnp.dot(minus.astype(jnp.float32), table[0].astype(jnp.float32), preferred_element_type=jnp.float32)
        for place, degree in enumerate(degrees):
            result[degree, azimuth] = real_part[:, place * channels:(place + 1) * channels]
            result[degree, -azimuth] = imag_part[:, place * channels:(place + 1) * channels]
    return result

def edge_message(source_rows, wig, gate, live, so2_zero, so2_one, so2_two):
    channels = gate.shape[1]
    shaped = source_rows.reshape(source_rows.shape[0], -1, channels)
    pieces = rotate_forward(shaped, wig)
    mixed = mix_orders(pieces, gate, so2_zero, so2_one, so2_two)
    message = rotate_back(mixed, wig).reshape(source_rows.shape[0], -1)
    return jnp.where(live[:, None], message, 0.0).astype(jnp.bfloat16)

def reference(features, box_atoms, edge_count, edge_tower, edge_plate, wigner, radial, so2_zero, so2_one, so2_two):
    span_x, span_y, span_z, atoms, feature_width = features.shape
    edges = edge_tower.shape[3]
    boxes = span_x * span_y * span_z
    flat_features = features.reshape(boxes * atoms, feature_width)
    tower_lists = edge_tower.reshape(boxes, edges)
    plate_lists = edge_plate.reshape(boxes, edges)
    counts = edge_count.reshape(boxes)
    rotations = wigner.reshape(boxes, wigner.shape[3], edges)
    gates = radial.reshape(boxes, edges, radial.shape[4])
    atom_ids = jnp.arange(atoms, dtype=jnp.int32)

    def device_step(summed, flat_index):
        box_x = flat_index // (span_y * span_z)
        box_y = flat_index // span_z % span_y
        box_z = flat_index % span_z
        tower_boxes = jnp.stack([(box_x + step_x) % span_x * span_y * span_z + box_y * span_z + box_z for step_x in (-1, 0, 1)])
        plate_boxes = jnp.stack([box_x * span_y * span_z + (box_y + step_y) % span_y * span_z + (box_z + step_z) % span_z for step_y in (-1, 0, 1) for step_z in (-1, 0, 1)])
        tower_atoms = (tower_boxes[:, None] * atoms + atom_ids[None, :]).reshape(-1).astype(jnp.int32)
        plate_atoms = (plate_boxes[:, None] * atoms + atom_ids[None, :]).reshape(-1).astype(jnp.int32)
        source_atom = tower_atoms[tower_lists[flat_index]]
        target_atom = plate_atoms[plate_lists[flat_index]]
        live = jnp.arange(edges, dtype=jnp.int32) < counts[flat_index]
        wig = rotations[flat_index]
        gate = gates[flat_index].astype(jnp.float32)
        to_plate = edge_message(flat_features[source_atom].astype(jnp.float32), wig, gate, live, so2_zero, so2_one, so2_two)
        to_tower = edge_message(flat_features[target_atom].astype(jnp.float32), wig, gate, live, so2_zero, so2_one, so2_two)
        summed = summed.at[target_atom].add(to_plate.astype(jnp.float32))
        summed = summed.at[source_atom].add(to_tower.astype(jnp.float32))
        return (summed, None)
    start = jnp.zeros((boxes * atoms, feature_width), jnp.float32)
    summed, unused = lax.scan(device_step, start, jnp.arange(boxes, dtype=jnp.int32))
    updated = flat_features.astype(jnp.float32) + summed
    updated = updated.reshape(span_x, span_y, span_z, atoms, feature_width)
    present = atom_ids[None, None, None, :] < box_atoms[..., None]
    return jnp.where(present[..., None], updated, 0.0).astype(jnp.bfloat16)
```

```python
import jax
import jax.numpy as jnp
from jax import lax
from jax.experimental import pallas as pl
from jax.experimental.pallas import tpu as pltpu
from jax.sharding import PartitionSpec as P

MESH = pl.DeviceIdType.MESH
DEGREE = 4
ORDER = 2
C = 128
A = 16
COEFS = 25
F = COEFS * C
F32 = jnp.float32
BF16 = jnp.bfloat16
NT = (((1,), (1,)), ((), ()))
TN = (((0,), (0,)), ((), ()))

WIG = {}
_at = 0
for _l in range(DEGREE + 1):
    for _m in range(-min(_l, ORDER), min(_l, ORDER) + 1):
        WIG[_l, _m] = _at
        _at += 2 * _l + 1
ROWS = _at

CHUNKS = (((4,), 16, 9), ((3,), 9, 7), ((0, 1, 2), 0, 9))
NCH = len(CHUNKS)
OWN = 4
XLOW, XHIGH = 9, 10


def kernel(
    feat_h, atoms_h, count_h, et_h, ep_h, wig_h, rad_h, w0_h, w1_h, w2_h,
    out,
    x, et, ep, wig, rad, w0, w1, w2, wb, gate, w0t, w1t, w2t, pick_t, pick_p,
    g, l0, l1, l2, y0, y1, y2, msg,
    sp, sc, ry, sz, rz, acc, st, tc, rt,
    atoms_s, count_s, local, fs, fr, bs, br,
):
    gx, gy, gz = lax.axis_index("gx"), lax.axis_index("gy"), lax.axis_index("gz")
    nx, ny, nz = lax.axis_size("gx"), lax.axis_size("gy"), lax.axis_size("gz")
    up = {"gx": lax.rem(gx + 1, nx), "gy": lax.rem(gy + 1, ny), "gz": lax.rem(gz + 1, nz)}
    down = {
        "gx": lax.rem(gx + nx - 1, nx),
        "gy": lax.rem(gy + ny - 1, ny),
        "gz": lax.rem(gz + nz - 1, nz),
    }

    def remote(src, dst, send, recv, axis, where):
        return pltpu.make_async_remote_copy(
            src_ref=src, dst_ref=dst, send_sem=send, recv_sem=recv,
            device_id={axis: where[axis]}, device_id_type=MESH,
        )

    loads = [
        pltpu.make_async_copy(src, dst, local.at[i])
        for i, (src, dst) in enumerate(
            (
                (feat_h, x.at[OWN]), (wig_h, wig), (et_h, et), (ep_h, ep), (rad_h, rad),
                (w0_h, w0), (w1_h, w1), (w2_h, w2), (atoms_h, atoms_s), (count_h, count_s),
            )
        )
    ]
    barrier = pltpu.get_barrier_semaphore()
    for axis in ("gx", "gy", "gz"):
        for where in (up, down):
            pl.semaphore_signal(
                barrier, inc=1, device_id={axis: where[axis]}, device_id_type=MESH
            )
    for load in loads:
        load.start()
    loads[0].wait()
    pl.semaphore_wait(barrier, 6)

    def forward(k, src, dst, axis, where):
        return remote(x.at[src], x.at[dst], fs.at[k], fr.at[k], axis, where)

    first = [
        forward(0, OWN, 3, "gz", up), forward(1, OWN, 5, "gz", down),
        forward(2, OWN, 1, "gy", up), forward(3, OWN, 7, "gy", down),
        forward(4, OWN, XLOW, "gx", up), forward(5, OWN, XHIGH, "gx", down),
    ]
    relays = [
        forward(6, 3, 0, "gy", up), forward(7, 3, 6, "gy", down),
        forward(8, 5, 2, "gy", up), forward(9, 5, 8, "gy", down),
    ]
    for copy in first:
        copy.start()

    for load in loads[1:]:
        load.wait()
    for o in range(ROWS):
        wb[o] = jnp.broadcast_to(wig[o], (8, wig.shape[2]))
    gate[...] = rad[...].T.astype(F32)
    live = lax.broadcasted_iota(jnp.int32, et.shape, 1) < count_s[0, 0]
    edges = et.shape[1]
    here_t = jnp.where(live, et[...], -1)
    here_p = jnp.where(live, ep[...], -1)
    pick_t[...] = (
        lax.broadcasted_iota(jnp.int32, (3 * A, edges), 0) == here_t
    ).astype(F32).astype(BF16)
    pick_p[...] = (
        lax.broadcasted_iota(jnp.int32, (9 * A, edges), 0) == here_p
    ).astype(F32).astype(BF16)

    def column(i):
        return pl.ds(pl.multiple_of(i * C, C), C)

    def turn0(i, c):
        w0t[column(i), :] = w0[:, column(i)].T
        return c

    def turn1(i, c):
        w1t[column(i), 0:512] = w1[1, :, column(i)].T
        w1t[column(i), 512:1024] = w1[0, :, column(i)].T
        return c

    def turn2(i, c):
        w2t[column(i), 0:384] = w2[1, :, column(i)].T
        w2t[column(i), 384:768] = w2[0, :, column(i)].T
        return c

    lax.fori_loop(0, 5, turn0, 0)
    lax.fori_loop(0, 4, turn1, 0)
    lax.fori_loop(0, 3, turn2, 0)

    def spread(o):
        row = wb[o]
        return jnp.concatenate([row, row], axis=0)

    def gather_tower(i, c):
        col = column(i)
        block = jnp.concatenate([x[XLOW, :, col], x[OWN, :, col], x[XHIGH, :, col]], axis=0)
        g[i] = lax.dot_general(block, pick_t[...], TN, preferred_element_type=F32)
        return c

    def gather_plate(i, c):
        block = x[0:9, :, column(i)].reshape(9 * A, C)
        g[i] = lax.dot_general(block, pick_p[...], TN, preferred_element_type=F32)
        return c

    def rotate(t, c):
        base = pl.multiple_of(t * 16, 16)
        tile = pl.ds(base, 16)
        scale = gate[tile, :]
        for l in range(DEGREE + 1):
            xs = [g[l * l + j, tile, :] for j in range(2 * l + 1)]
            for m in range(-min(l, ORDER), min(l, ORDER) + 1):
                total = spread(WIG[l, m]) * xs[0]
                for j in range(1, 2 * l + 1):
                    total = total + spread(WIG[l, m] + j) * xs[j]
                low = (total * scale).astype(BF16)
                if m == 0:
                    l0[pl.ds(base + l * C, 16), :] = low
                else:
                    ref, size = (l1, 4 * C) if abs(m) == 1 else (l2, 3 * C)
                    at = base + (l - abs(m)) * C
                    if m > 0:
                        ref[pl.ds(at + size, 16), :] = low
                    else:
                        ref[pl.ds(at, 16), :] = -low
                        ref[pl.ds(at + 2 * size, 16), :] = low
        return c

    def mix():
        y0[...] = jnp.dot(w0t[...], l0[...], preferred_element_type=F32)
        y1[0] = jnp.dot(w1t[...], l1[0:1024, :], preferred_element_type=F32)
        y1[1] = jnp.dot(w1t[...], l1[512:1536, :], preferred_element_type=F32)
        y2[0] = jnp.dot(w2t[...], l2[0:768, :], preferred_element_type=F32)
        y2[1] = jnp.dot(w2t[...], l2[384:1152, :], preferred_element_type=F32)

    def rotate_back(degrees):
        def step(t, c):
            base = pl.multiple_of(t * 16, 16)
            for l in degrees:
                within = min(l, ORDER)
                ys = {}
                for m in range(-within, within + 1):
                    if m == 0:
                        ys[m] = y0[pl.ds(base + l * C, 16), :]
                    else:
                        ref = y1 if abs(m) == 1 else y2
                        ys[m] = ref[0 if m > 0 else 1, pl.ds(base + (l - abs(m)) * C, 16), :]
                for j in range(2 * l + 1):
                    total = None
                    for m in range(-within, within + 1):
                        term = spread(WIG[l, m] + j) * ys[m]
                        total = term if total is None else total + term
                    msg[l * l + j, pl.ds(base, 16), :] = total.astype(BF16)
            return c

        lax.fori_loop(0, 8, step, 0)

    def chunk_cols(q):
        return pl.ds(CHUNKS[q][1] * C, CHUNKS[q][2] * C)

    def back(q, part, axis, where):
        cols = chunk_cols(q)
        side = 0 if where is down else 1
        k = q * 6 + part * 2 + side
        src, dst = ((sp, ry), (sz, rz), (st, rt))[part]
        index = (side, slice(None), slice(None), cols) if part == 0 else (side, slice(None), cols)
        return remote(src.at[index], dst.at[index], bs.at[k], br.at[k], axis, where)

    backs = [
        [[back(q, part, axis, where) for where in (down, up)]
         for part, axis in enumerate(("gy", "gz", "gx"))]
        for q in range(NCH)
    ]

    def along(q):
        cols = chunk_cols(q)
        for copy in backs[q][0]:
            copy.wait_recv()
        for f in (0, 2):
            total = sc[f, :, cols] + ry[0, f, :, cols].astype(F32) + ry[1, f, :, cols].astype(F32)
            sz[f // 2, :, cols] = total.astype(BF16)
        for copy in backs[q][1]:
            copy.start()
        acc[:, cols] = sc[1, :, cols] + ry[0, 1, :, cols].astype(F32) + ry[1, 1, :, cols].astype(F32)

    first[0].wait_recv()
    relays[0].start()
    relays[1].start()
    first[1].wait_recv()
    relays[2].start()
    relays[3].start()

    first[4].wait_recv()
    first[5].wait_recv()
    lax.fori_loop(0, COEFS, gather_tower, 0, unroll=5)
    lax.fori_loop(0, 8, rotate, 0)
    mix()
    for q, (degrees, low, many) in enumerate(CHUNKS):
        rotate_back(degrees)

        def scatter_plate(i, c):
            s = lax.dot_general(pick_p[...], msg[i], NT, preferred_element_type=F32)
            col = column(i)
            for f in range(3):
                sp[0, f, :, col] = s[f * A : (f + 1) * A].astype(BF16)
                sc[f, :, col] = s[(3 + f) * A : (4 + f) * A]
                sp[1, f, :, col] = s[(6 + f) * A : (7 + f) * A].astype(BF16)
            return c

        lax.fori_loop(low, low + many, scatter_plate, 0)
        for copy in backs[q][0]:
            copy.start()

    for copy in first[2:4] + relays:
        copy.wait_recv()
    lax.fori_loop(0, COEFS, gather_plate, 0, unroll=5)
    lax.fori_loop(0, 8, rotate, 0)
    along(0)
    mix()
    along(1)
    along(2)
    for q, (degrees, low, many) in enumerate(CHUNKS):
        rotate_back(degrees)

        def scatter_tower(i, c):
            s = lax.dot_general(pick_t[...], msg[i], NT, preferred_element_type=F32)
            col = column(i)
            st[0, :, col] = s[0:A].astype(BF16)
            tc[:, col] = s[A : 2 * A]
            st[1, :, col] = s[2 * A : 3 * A].astype(BF16)
            return c

        lax.fori_loop(low, low + many, scatter_tower, 0)
        for copy in backs[q][2]:
            copy.start()

    present = lax.broadcasted_iota(jnp.int32, (A, C), 0) < atoms_s[0, 0]
    for q, (degrees, low, many) in enumerate(CHUNKS):
        for copy in backs[q][1] + backs[q][2]:
            copy.wait_recv()

        def finish(i, c):
            col = column(i)
            total = (
                tc[:, col] + rt[0, :, col].astype(F32) + rt[1, :, col].astype(F32)
                + acc[:, col] + rz[0, :, col].astype(F32) + rz[1, :, col].astype(F32)
                + x[OWN, :, col].astype(F32)
            )
            out[:, col] = jnp.where(present, total, 0.0).astype(BF16)
            return c

        lax.fori_loop(low, low + many, finish, 0)
    for copy in first + relays:
        copy.wait_send()
    for q in range(NCH):
        for part in backs[q]:
            for copy in part:
                copy.wait_send()


def body(features, box_atoms, edge_count, edge_tower, edge_plate, wigner, radial, so2_zero, so2_one, so2_two):
    E = edge_tower.shape[3]
    hbm = pl.BlockSpec(memory_space=pl.ANY)
    V = pltpu.VMEM
    dma = pltpu.SemaphoreType.DMA
    result = pl.pallas_call(
        kernel,
        out_shape=jax.ShapeDtypeStruct((A, F), BF16),
        in_specs=[hbm] * 10,
        out_specs=pl.BlockSpec(memory_space=pltpu.VMEM),
        scratch_shapes=[
            V((11, A, F), BF16), V((1, E), jnp.int32), V((1, E), jnp.int32), V((ROWS, 1, E), F32),
            V((E, C), BF16), V((640, 640), BF16), V((2, 512, 512), BF16), V((2, 384, 384), BF16),
            V((ROWS, 8, E), F32), V((C, E), F32),
            V((640, 640), BF16), V((512, 1024), BF16), V((384, 768), BF16),
            V((3 * A, E), BF16), V((9 * A, E), BF16),
            V((COEFS, C, E), F32), V((640, E), BF16), V((1536, E), BF16), V((1152, E), BF16),
            V((640, E), F32), V((2, 512, E), F32), V((2, 384, E), F32), V((COEFS, C, E), BF16),
            V((2, 3, A, F), BF16), V((3, A, F), F32), V((2, 3, A, F), BF16),
            V((2, A, F), BF16), V((2, A, F), BF16), V((A, F), F32),
            V((2, A, F), BF16), V((A, F), F32), V((2, A, F), BF16),
            pltpu.SMEM((1, 1), jnp.int32), pltpu.SMEM((1, 1), jnp.int32), dma((10,)), dma((10,)), dma((10,)), dma((6 * NCH,)), dma((6 * NCH,)),
        ],
        compiler_params=pltpu.CompilerParams(collective_id=0, has_side_effects=True),
        name="layer",
    )(
        features.reshape(A, F), box_atoms.reshape(1, 1), edge_count.reshape(1, 1),
        edge_tower.reshape(1, E), edge_plate.reshape(1, E),
        wigner.reshape(ROWS, 1, E), radial.reshape(E, C), so2_zero, so2_one, so2_two,
    )
    return result.reshape(features.shape)


def solution(mesh):
    boxes = ("gx", "gy", "gz")
    placed = (
        P(*boxes, None, None), P(*boxes), P(*boxes), P(*boxes, None), P(*boxes, None),
        P(*boxes, None, None), P(*boxes, None, None), P(), P(), P(),
    )
    return jax.shard_map(
        body, mesh=mesh, in_specs=placed, out_specs=P(*boxes, None, None), check_vma=False
    )
```

```python
import jax
import jax.numpy as jnp
from jax import lax
from jax.experimental import pallas as pl
from jax.experimental.pallas import tpu as pltpu
from jax.sharding import PartitionSpec as P

MESH = pl.DeviceIdType.MESH
DEGREE = 4
ORDER = 2
C = 128
A = 16
COEFS = 25
F = COEFS * C
F32 = jnp.float32
BF16 = jnp.bfloat16
NT = (((1,), (1,)), ((), ()))
TN = (((0,), (0,)), ((), ()))

WIG = {}
_at = 0
for _l in range(DEGREE + 1):
    for _m in range(-min(_l, ORDER), min(_l, ORDER) + 1):
        WIG[_l, _m] = _at
        _at += 2 * _l + 1
ROWS = _at

CHUNKS = (((4,), 16, 9), ((3,), 9, 7), ((0, 1, 2), 0, 9))
NCH = len(CHUNKS)
OWN = 4
XLOW, XHIGH = 9, 10


def kernel(
    feat_h, atoms_h, count_h, et_h, ep_h, wig_h, rad_h, w0_h, w1_h, w2_h,
    out,
    x, et, ep, wig, rad, w0, w1, w2, wb, gate, w0t, w1t, w2t, pick_t, pick_p,
    g, l0, l1, l2, y0, y1, y2, msg,
    sp, sc, ry, sz, rz, st, tc, rt,
    atoms_s, count_s, local, fs, fr, bs, br,
):
    E = et.shape[1]
    gx, gy, gz = lax.axis_index("gx"), lax.axis_index("gy"), lax.axis_index("gz")
    nx, ny, nz = lax.axis_size("gx"), lax.axis_size("gy"), lax.axis_size("gz")
    up = {"gx": lax.rem(gx + 1, nx), "gy": lax.rem(gy + 1, ny), "gz": lax.rem(gz + 1, nz)}
    down = {
        "gx": lax.rem(gx + nx - 1, nx),
        "gy": lax.rem(gy + ny - 1, ny),
        "gz": lax.rem(gz + nz - 1, nz),
    }

    def remote(src, dst, send, recv, axis, where):
        return pltpu.make_async_remote_copy(
            src_ref=src, dst_ref=dst, send_sem=send, recv_sem=recv,
            device_id={axis: where[axis]}, device_id_type=MESH,
        )

    loads = [
        pltpu.make_async_copy(src, dst, local.at[i])
        for i, (src, dst) in enumerate(
            (
                (feat_h, x.at[OWN]), (wig_h, wig), (et_h, et), (ep_h, ep), (rad_h, rad),
                (w0_h, w0), (w1_h, w1), (w2_h, w2), (atoms_h, atoms_s), (count_h, count_s),
            )
        )
    ]
    barrier = pltpu.get_barrier_semaphore()
    for axis in ("gx", "gy", "gz"):
        for where in (up, down):
            pl.semaphore_signal(
                barrier, inc=1, device_id={axis: where[axis]}, device_id_type=MESH
            )
    for load in loads:
        load.start()
    loads[0].wait()
    pl.semaphore_wait(barrier, 6)

    def forward(k, src, dst, axis, where):
        return remote(x.at[src], x.at[dst], fs.at[k], fr.at[k], axis, where)

    first = [
        forward(0, OWN, 3, "gz", up), forward(1, OWN, 5, "gz", down),
        forward(2, OWN, 1, "gy", up), forward(3, OWN, 7, "gy", down),
        forward(4, OWN, XLOW, "gx", up), forward(5, OWN, XHIGH, "gx", down),
    ]
    relays = [
        forward(6, 3, 0, "gy", up), forward(7, 5, 8, "gy", down),
        forward(8, 7, 6, "gz", up), forward(9, 1, 2, "gz", down),
    ]
    for copy in first:
        copy.start()

    for load in loads[1:]:
        load.wait()
    for o in range(ROWS):
        wb[o] = jnp.broadcast_to(wig[o], (8, wig.shape[2]))
    gate[...] = rad[...].T.astype(F32)
    live = lax.broadcasted_iota(jnp.int32, et.shape, 1) < count_s[0, 0]
    edges = et.shape[1]
    here_t = jnp.where(live, et[...], -1)
    here_p = jnp.where(live, ep[...], -1)
    pick_t[...] = (
        lax.broadcasted_iota(jnp.int32, (3 * A, edges), 0) == here_t
    ).astype(F32).astype(BF16)
    pick_p[...] = (
        lax.broadcasted_iota(jnp.int32, (9 * A, edges), 0) == here_p
    ).astype(F32).astype(BF16)

    def column(i):
        return pl.ds(pl.multiple_of(i * C, C), C)

    def turn0(i, c):
        w0t[column(i), :] = w0[:, column(i)].T
        return c

    def turn1(i, c):
        w1t[column(i), 0:512] = w1[1, :, column(i)].T
        w1t[column(i), 512:1024] = w1[0, :, column(i)].T
        return c

    def turn2(i, c):
        w2t[column(i), 0:384] = w2[1, :, column(i)].T
        w2t[column(i), 384:768] = w2[0, :, column(i)].T
        return c

    lax.fori_loop(0, 5, turn0, 0)
    lax.fori_loop(0, 4, turn1, 0)
    lax.fori_loop(0, 3, turn2, 0)

    def spread(o):
        row = wb[o]
        return jnp.concatenate([row, row], axis=0)

    def gather_tower(i, c):
        col = column(i)
        block = jnp.concatenate([x[XLOW, :, col], x[OWN, :, col], x[XHIGH, :, col]], axis=0)
        g[i] = lax.dot_general(block, pick_t[...], TN, preferred_element_type=F32)
        return c

    def gather_plate(i, c):
        block = x[0:9, :, column(i)].reshape(9 * A, C)
        g[i] = lax.dot_general(block, pick_p[...], TN, preferred_element_type=F32)
        return c

    def rotate(t, c):
        base = pl.multiple_of(t * 16, 16)
        tile = pl.ds(base, 16)
        scale = gate[tile, :]
        for l in range(DEGREE + 1):
            xs = [g[l * l + j, tile, :] for j in range(2 * l + 1)]
            for m in range(-min(l, ORDER), min(l, ORDER) + 1):
                total = spread(WIG[l, m]) * xs[0]
                for j in range(1, 2 * l + 1):
                    total = total + spread(WIG[l, m] + j) * xs[j]
                low = (total * scale).astype(BF16)
                if m == 0:
                    l0[pl.ds(base + l * C, 16), :] = low
                else:
                    ref, size = (l1, 4 * C) if abs(m) == 1 else (l2, 3 * C)
                    at = base + (l - abs(m)) * C
                    if m > 0:
                        ref[pl.ds(at + size, 16), 0:E] = low
                        ref[pl.ds(at, 16), E : 2 * E] = low
                    else:
                        ref[pl.ds(at, 16), 0:E] = -low
                        ref[pl.ds(at + size, 16), E : 2 * E] = low
        return c

    def mix():
        y0[...] = jnp.dot(w0t[...], l0[...], preferred_element_type=F32)
        y1[...] = jnp.dot(w1t[...], l1[...], preferred_element_type=F32)
        y2[...] = jnp.dot(w2t[...], l2[...], preferred_element_type=F32)

    def rotate_back(degrees):
        def step(t, c):
            base = pl.multiple_of(t * 16, 16)
            for l in degrees:
                within = min(l, ORDER)
                ys = {}
                for m in range(-within, within + 1):
                    if m == 0:
                        ys[m] = y0[pl.ds(base + l * C, 16), :]
                    else:
                        ref = y1 if abs(m) == 1 else y2
                        lanes = slice(0, E) if m > 0 else slice(E, 2 * E)
                        ys[m] = ref[pl.ds(base + (l - abs(m)) * C, 16), lanes]
                for j in range(2 * l + 1):
                    total = None
                    for m in range(-within, within + 1):
                        term = spread(WIG[l, m] + j) * ys[m]
                        total = term if total is None else total + term
                    msg[l * l + j, pl.ds(base, 16), :] = total.astype(BF16)
            return c

        lax.fori_loop(0, 8, step, 0)

    def chunk_cols(q):
        return pl.ds(CHUNKS[q][1] * C, CHUNKS[q][2] * C)

    def back(q, part, i, axis, where):
        cols = chunk_cols(q)
        src, dst = ((sp, ry), (sz, rz), (st, rt))[part]
        k = q * 10 + part * 4 + i
        return remote(
            src.at[i, :, cols], dst.at[i, :, cols], bs.at[k], br.at[k], axis, where
        )

    routes = (
        (("gy", down), ("gz", up), ("gz", down), ("gy", up)),
        (("gy", down), ("gz", down), ("gz", up), ("gy", up)),
        (("gx", down), ("gx", up)),
    )
    backs = [
        [[back(q, part, i, *route) for i, route in enumerate(routes[part])] for part in range(3)]
        for q in range(NCH)
    ]

    def along(q):
        cols = chunk_cols(q)
        for side, corner in ((1, 0), (0, 1), (3, 2), (2, 3)):
            backs[q][0][corner].wait_recv()
            sz[side, :, cols] = (sc[side, :, cols] + ry[corner, :, cols].astype(F32)).astype(BF16)
            backs[q][1][side].start()

    first[3].wait_recv()
    relays[2].start()
    first[2].wait_recv()
    relays[3].start()

    first[4].wait_recv()
    first[5].wait_recv()
    lax.fori_loop(0, COEFS, gather_tower, 0, unroll=True)
    first[0].wait_recv()
    relays[0].start()
    first[1].wait_recv()
    relays[1].start()
    lax.fori_loop(0, 8, rotate, 0)
    mix()
    for q, (degrees, low, many) in enumerate(CHUNKS):
        rotate_back(degrees)

        for i in range(low, low + many):
            s = lax.dot_general(pick_p[...], msg[i], NT, preferred_element_type=F32)
            col = pl.ds(i * C, C)
            for k, p in enumerate((0, 2, 6, 8)):
                sp[k, :, col] = s[p * A : (p + 1) * A].astype(BF16)
            for k, p in enumerate((1, 3, 5, 7, 4)):
                sc[k, :, col] = s[p * A : (p + 1) * A]
        for copy in backs[q][0]:
            copy.start()

    for copy in relays:
        copy.wait_recv()
    lax.fori_loop(0, COEFS, gather_plate, 0, unroll=True)
    lax.fori_loop(0, 8, rotate, 0)
    along(0)
    mix()
    along(1)
    for q, (degrees, low, many) in enumerate(CHUNKS):
        rotate_back(degrees)

        for i in range(low, low + many):
            s = lax.dot_general(pick_t[...], msg[i], NT, preferred_element_type=F32)
            col = pl.ds(i * C, C)
            st[0, :, col] = s[0:A].astype(BF16)
            tc[:, col] = s[A : 2 * A]
            st[1, :, col] = s[2 * A : 3 * A].astype(BF16)
        for copy in backs[q][2]:
            copy.start()
        if q == 0:
            along(2)

    present = lax.broadcasted_iota(jnp.int32, (A, C), 0) < atoms_s[0, 0]
    for q, (degrees, low, many) in enumerate(CHUNKS):
        for copy in backs[q][1] + backs[q][2]:
            copy.wait_recv()

        def finish(i, c):
            col = column(i)
            total = (
                tc[:, col] + rt[0, :, col].astype(F32) + rt[1, :, col].astype(F32)
                + sc[4, :, col] + rz[0, :, col].astype(F32) + rz[1, :, col].astype(F32)
                + rz[2, :, col].astype(F32) + rz[3, :, col].astype(F32)
                + x[OWN, :, col].astype(F32)
            )
            out[:, col] = jnp.where(present, total, 0.0).astype(BF16)
            return c

        lax.fori_loop(low, low + many, finish, 0)
    for copy in first + relays:
        copy.wait_send()
    for q in range(NCH):
        for part in backs[q]:
            for copy in part:
                copy.wait_send()


def body(features, box_atoms, edge_count, edge_tower, edge_plate, wigner, radial, so2_zero, so2_one, so2_two):
    E = edge_tower.shape[3]
    hbm = pl.BlockSpec(memory_space=pl.ANY)
    V = pltpu.VMEM
    dma = pltpu.SemaphoreType.DMA
    result = pl.pallas_call(
        kernel,
        out_shape=jax.ShapeDtypeStruct((A, F), BF16),
        in_specs=[hbm] * 10,
        out_specs=pl.BlockSpec(memory_space=pltpu.VMEM),
        scratch_shapes=[
            V((11, A, F), BF16), V((1, E), jnp.int32), V((1, E), jnp.int32), V((ROWS, 1, E), F32),
            V((E, C), BF16), V((640, 640), BF16), V((2, 512, 512), BF16), V((2, 384, 384), BF16),
            V((ROWS, 8, E), F32), V((C, E), F32),
            V((640, 640), BF16), V((512, 1024), BF16), V((384, 768), BF16),
            V((3 * A, E), BF16), V((9 * A, E), BF16),
            V((COEFS, C, E), F32), V((640, E), BF16), V((1024, 2 * E), BF16), V((768, 2 * E), BF16),
            V((640, E), F32), V((512, 2 * E), F32), V((384, 2 * E), F32), V((COEFS, C, E), BF16),
            V((4, A, F), BF16), V((5, A, F), F32), V((4, A, F), BF16),
            V((4, A, F), BF16), V((4, A, F), BF16),
            V((2, A, F), BF16), V((A, F), F32), V((2, A, F), BF16),
            pltpu.SMEM((1, 1), jnp.int32), pltpu.SMEM((1, 1), jnp.int32), dma((10,)), dma((10,)), dma((10,)), dma((10 * NCH,)), dma((10 * NCH,)),
        ],
        compiler_params=pltpu.CompilerParams(
            collective_id=0, has_side_effects=True
        ),
        name="layer",
    )(
        features.reshape(A, F), box_atoms.reshape(1, 1), edge_count.reshape(1, 1),
        edge_tower.reshape(1, E), edge_plate.reshape(1, E),
        wigner.reshape(ROWS, 1, E), radial.reshape(E, C), so2_zero, so2_one, so2_two,
    )
    return result.reshape(features.shape)


def solution(mesh):
    boxes = ("gx", "gy", "gz")
    placed = (
        P(*boxes, None, None), P(*boxes), P(*boxes), P(*boxes, None), P(*boxes, None),
        P(*boxes, None, None), P(*boxes, None, None), P(), P(), P(),
    )
    return jax.shard_map(
        body, mesh=mesh, in_specs=placed, out_specs=P(*boxes, None, None), check_vma=False
    )
```

```python
import jax
import jax.numpy as jnp
from jax import lax
from jax.experimental import pallas as pl
from jax.experimental.pallas import tpu as pltpu
from jax.sharding import PartitionSpec as P

MESH = pl.DeviceIdType.MESH
DEGREE = 4
ORDER = 2
C = 128
A = 16
COEFS = 25
F = COEFS * C
F32 = jnp.float32
BF16 = jnp.bfloat16
NT = (((1,), (1,)), ((), ()))
TN = (((0,), (0,)), ((), ()))

WIG = {}
_at = 0
for _l in range(DEGREE + 1):
    for _m in range(-min(_l, ORDER), min(_l, ORDER) + 1):
        WIG[_l, _m] = _at
        _at += 2 * _l + 1
ROWS = _at

CHUNKS = (((4,), 16, 9), ((3,), 9, 7), ((0, 1, 2), 0, 9))
NCH = len(CHUNKS)
HALVES = ((0, 13 * C), (13 * C, 12 * C))
OWN = 4
XLOW, XHIGH = 9, 10


def kernel(
    feat_h, atoms_h, count_h, et_h, ep_h, wig_h, rad_h, w0_h, w1_h, w2_h,
    out,
    x, et, ep, wig, rad, w0, w1, w2, wb, gate, w0t, w1t, w2t, pick_t, pick_p,
    g, l0, l1, l2, y0, y1, y2, msg,
    sp, sc, ry, sz, rz, st, tc, rt,
    atoms_s, count_s, local, fs, fr, bs, br,
):
    E = et.shape[1]
    gx, gy, gz = lax.axis_index("gx"), lax.axis_index("gy"), lax.axis_index("gz")
    nx, ny, nz = lax.axis_size("gx"), lax.axis_size("gy"), lax.axis_size("gz")
    up = {"gx": lax.rem(gx + 1, nx), "gy": lax.rem(gy + 1, ny), "gz": lax.rem(gz + 1, nz)}
    down = {
        "gx": lax.rem(gx + nx - 1, nx),
        "gy": lax.rem(gy + ny - 1, ny),
        "gz": lax.rem(gz + nz - 1, nz),
    }

    def remote(src, dst, send, recv, axis, where):
        return pltpu.make_async_remote_copy(
            src_ref=src, dst_ref=dst, send_sem=send, recv_sem=recv,
            device_id={axis: where[axis]}, device_id_type=MESH,
        )

    loads = [
        pltpu.make_async_copy(src, dst, local.at[i])
        for i, (src, dst) in enumerate(
            (
                (feat_h, x.at[OWN]), (wig_h, wig), (et_h, et), (ep_h, ep), (rad_h, rad),
                (w0_h, w0), (w1_h, w1), (w2_h, w2), (atoms_h, atoms_s), (count_h, count_s),
            )
        )
    ]
    barrier = pltpu.get_barrier_semaphore()
    for axis in ("gx", "gy", "gz"):
        for where in (up, down):
            pl.semaphore_signal(
                barrier, inc=1, device_id={axis: where[axis]}, device_id_type=MESH
            )
    for load in loads:
        load.start()
    loads[0].wait()
    pl.semaphore_wait(barrier, 6)

    def forward(k, src, dst, axis, where, half=None):
        if half is None:
            return remote(x.at[src], x.at[dst], fs.at[k], fr.at[k], axis, where)
        cols = pl.ds(*HALVES[half])
        k = k + 10 * half
        return remote(x.at[src, :, cols], x.at[dst, :, cols], fs.at[k], fr.at[k], axis, where)

    first = [
        [
            forward(0, OWN, 3, "gz", up, h), forward(1, OWN, 5, "gz", down, h),
            forward(2, OWN, 1, "gy", up, h), forward(3, OWN, 7, "gy", down, h),
        ]
        for h in range(2)
    ]
    towers = [forward(4, OWN, XLOW, "gx", up), forward(5, OWN, XHIGH, "gx", down)]
    relays = [
        [
            forward(6, 3, 0, "gy", up, h), forward(7, 5, 8, "gy", down, h),
            forward(9, 1, 2, "gz", down, h), forward(8, 7, 6, "gz", up, h),
        ]
        for h in range(2)
    ]
    for copy in towers + first[0] + first[1]:
        copy.start()

    def pass_on(half):
        for i in (2, 3, 0, 1):
            first[half][i].wait_recv()
            relays[half][i].start()

    for load in loads[1:]:
        load.wait()
    for o in range(ROWS):
        wb[o] = jnp.broadcast_to(wig[o], (8, wig.shape[2]))
    gate[...] = rad[...].T.astype(F32)
    live = lax.broadcasted_iota(jnp.int32, et.shape, 1) < count_s[0, 0]
    edges = et.shape[1]
    here_t = jnp.where(live, et[...], -1)
    here_p = jnp.where(live, ep[...], -1)
    pick_t[...] = (
        lax.broadcasted_iota(jnp.int32, (3 * A, edges), 0) == here_t
    ).astype(F32).astype(BF16)
    pick_p[...] = (
        lax.broadcasted_iota(jnp.int32, (9 * A, edges), 0) == here_p
    ).astype(F32).astype(BF16)

    def column(i):
        return pl.ds(pl.multiple_of(i * C, C), C)

    def turn0(i, c):
        for k in range(5):
            w0t[k, column(i), :] = w0[k * C : (k + 1) * C, column(i)].T
        return c

    def turn1(i, c):
        for k in range(4):
            w1t[k, column(i), :] = w1[1, k * C : (k + 1) * C, column(i)].T
            w1t[4 + k, column(i), :] = w1[0, k * C : (k + 1) * C, column(i)].T
        return c

    def turn2(i, c):
        for k in range(3):
            w2t[k, column(i), :] = w2[1, k * C : (k + 1) * C, column(i)].T
            w2t[3 + k, column(i), :] = w2[0, k * C : (k + 1) * C, column(i)].T
        return c

    lax.fori_loop(0, 5, turn0, 0)
    lax.fori_loop(0, 4, turn1, 0)
    lax.fori_loop(0, 3, turn2, 0)

    def spread(o):
        row = wb[o]
        return jnp.concatenate([row, row], axis=0)

    def gather_tower(i, c):
        col = column(i)
        block = jnp.concatenate([x[XLOW, :, col], x[OWN, :, col], x[XHIGH, :, col]], axis=0)
        g[i] = lax.dot_general(block, pick_t[...], TN, preferred_element_type=F32)
        return c

    def gather_plate(i, c):
        block = x[0:9, :, column(i)].reshape(9 * A, C)
        g[i] = lax.dot_general(block, pick_p[...], TN, preferred_element_type=F32)
        return c

    def rotate(t, c):
        base = pl.multiple_of(t * 16, 16)
        tile = pl.ds(base, 16)
        scale = gate[tile, :]
        for l in range(DEGREE + 1):
            xs = [g[l * l + j, tile, :] for j in range(2 * l + 1)]
            for m in range(-min(l, ORDER), min(l, ORDER) + 1):
                total = spread(WIG[l, m]) * xs[0]
                for j in range(1, 2 * l + 1):
                    total = total + spread(WIG[l, m] + j) * xs[j]
                low = (total * scale).astype(BF16)
                if m == 0:
                    l0[pl.ds(base + l * C, 16), :] = low
                else:
                    ref, size = (l1, 4 * C) if abs(m) == 1 else (l2, 3 * C)
                    at = base + (l - abs(m)) * C
                    if m > 0:
                        ref[pl.ds(at + size, 16), 0:E] = low
                        ref[pl.ds(at, 16), E : 2 * E] = low
                    else:
                        ref[pl.ds(at, 16), 0:E] = -low
                        ref[pl.ds(at + size, 16), E : 2 * E] = low
        return c

    def mix():
        for y, w, low in ((y0, w0t, l0), (y1, w1t, l1), (y2, w2t, l2)):
            table = jnp.concatenate([w[k] for k in range(w.shape[0])], axis=1)
            y[...] = jnp.dot(table, low[...], preferred_element_type=F32)

    def rotate_back(degrees):
        def step(t, c):
            base = pl.multiple_of(t * 16, 16)
            for l in degrees:
                within = min(l, ORDER)
                ys = {}
                for m in range(-within, within + 1):
                    if m == 0:
                        ys[m] = y0[pl.ds(base + l * C, 16), :]
                    else:
                        ref = y1 if abs(m) == 1 else y2
                        lanes = slice(0, E) if m > 0 else slice(E, 2 * E)
                        ys[m] = ref[pl.ds(base + (l - abs(m)) * C, 16), lanes]
                for j in range(2 * l + 1):
                    total = None
                    for m in range(-within, within + 1):
                        term = spread(WIG[l, m] + j) * ys[m]
                        total = term if total is None else total + term
                    msg[l * l + j, pl.ds(base, 16), :] = total.astype(BF16)
            return c

        lax.fori_loop(0, 8, step, 0)

    def chunk_cols(q):
        return pl.ds(CHUNKS[q][1] * C, CHUNKS[q][2] * C)

    def back(q, part, i, axis, where):
        cols = chunk_cols(q)
        src, dst = ((sp, ry), (sz, rz), (st, rt))[part]
        k = q * 10 + part * 4 + i
        return remote(
            src.at[i, :, cols], dst.at[i, :, cols], bs.at[k], br.at[k], axis, where
        )

    routes = (
        (("gy", down), ("gz", up), ("gz", down), ("gy", up)),
        (("gy", down), ("gz", down), ("gz", up), ("gy", up)),
        (("gx", down), ("gx", up)),
    )
    backs = [
        [[back(q, part, i, *route) for i, route in enumerate(routes[part])] for part in range(3)]
        for q in range(NCH)
    ]

    def along(q):
        cols = chunk_cols(q)
        for side, corner in ((1, 0), (0, 1), (3, 2), (2, 3)):
            backs[q][0][corner].wait_recv()
            sz[side, :, cols] = (sc[side, :, cols] + ry[corner, :, cols].astype(F32)).astype(BF16)
            backs[q][1][side].start()

    pass_on(0)
    for copy in towers:
        copy.wait_recv()
    lax.fori_loop(0, COEFS, gather_tower, 0, unroll=True)
    pass_on(1)
    lax.fori_loop(0, 8, rotate, 0)
    mix()
    for q, (degrees, low, many) in enumerate(CHUNKS):
        rotate_back(degrees)

        for i in range(low, low + many):
            s = lax.dot_general(pick_p[...], msg[i], NT, preferred_element_type=F32)
            col = pl.ds(i * C, C)
            for k, p in enumerate((0, 2, 6, 8)):
                sp[k, :, col] = s[p * A : (p + 1) * A].astype(BF16)
            for k, p in enumerate((1, 3, 5, 7, 4)):
                sc[k, :, col] = s[p * A : (p + 1) * A]
        for copy in backs[q][0]:
            copy.start()

    for copy in relays[0] + relays[1]:
        copy.wait_recv()
    lax.fori_loop(0, COEFS, gather_plate, 0, unroll=True)
    lax.fori_loop(0, 8, rotate, 0)
    along(0)
    mix()
    along(1)
    for q, (degrees, low, many) in enumerate(CHUNKS):
        rotate_back(degrees)

        for i in range(low, low + many):
            s = lax.dot_general(pick_t[...], msg[i], NT, preferred_element_type=F32)
            col = pl.ds(i * C, C)
            st[0, :, col] = s[0:A].astype(BF16)
            tc[:, col] = s[A : 2 * A]
            st[1, :, col] = s[2 * A : 3 * A].astype(BF16)
        for copy in backs[q][2]:
            copy.start()
        if q == 0:
            along(2)

    for q in range(NCH):
        for copy in backs[q][1] + backs[q][2]:
            copy.wait_recv()

        cols = chunk_cols(q)
        present = lax.broadcasted_iota(jnp.int32, (A, CHUNKS[q][2] * C), 0) < atoms_s[0, 0]
        total = tc[:, cols] + sc[4, :, cols] + x[OWN, :, cols].astype(F32)
        for ref, parts in ((rt, 2), (rz, 4)):
            for i in range(parts):
                total = total + ref[i, :, cols].astype(F32)
        out[:, cols] = jnp.where(present, total, 0.0).astype(BF16)
    for copy in first[0] + first[1] + towers + relays[0] + relays[1]:
        copy.wait_send()
    for q in range(NCH):
        for part in backs[q]:
            for copy in part:
                copy.wait_send()


def body(features, box_atoms, edge_count, edge_tower, edge_plate, wigner, radial, so2_zero, so2_one, so2_two):
    E = edge_tower.shape[3]
    hbm = pl.BlockSpec(memory_space=pl.ANY)
    V = pltpu.VMEM
    dma = pltpu.SemaphoreType.DMA
    result = pl.pallas_call(
        kernel,
        out_shape=jax.ShapeDtypeStruct((A, F), BF16),
        in_specs=[hbm] * 10,
        out_specs=pl.BlockSpec(memory_space=pltpu.VMEM),
        scratch_shapes=[
            V((11, A, F), BF16), V((1, E), jnp.int32), V((1, E), jnp.int32), V((ROWS, 1, E), F32),
            V((E, C), BF16), V((640, 640), BF16), V((2, 512, 512), BF16), V((2, 384, 384), BF16),
            V((ROWS, 8, E), F32), V((C, E), F32),
            V((5, 640, C), BF16), V((8, 512, C), BF16), V((6, 384, C), BF16),
            V((3 * A, E), BF16), V((9 * A, E), BF16),
            V((COEFS, C, E), F32), V((640, E), BF16), V((1024, 2 * E), BF16), V((768, 2 * E), BF16),
            V((640, E), F32), V((512, 2 * E), F32), V((384, 2 * E), F32), V((COEFS, C, E), BF16),
            V((4, A, F), BF16), V((5, A, F), F32), V((4, A, F), BF16),
            V((4, A, F), BF16), V((4, A, F), BF16),
            V((2, A, F), BF16), V((A, F), F32), V((2, A, F), BF16),
            pltpu.SMEM((1, 1), jnp.int32), pltpu.SMEM((1, 1), jnp.int32), dma((10,)), dma((20,)), dma((20,)), dma((10 * NCH,)), dma((10 * NCH,)),
        ],
        compiler_params=pltpu.CompilerParams(
            collective_id=0, has_side_effects=True
        ),
        name="layer",
    )(
        features.reshape(A, F), box_atoms.reshape(1, 1), edge_count.reshape(1, 1),
        edge_tower.reshape(1, E), edge_plate.reshape(1, E),
        wigner.reshape(ROWS, 1, E), radial.reshape(E, C), so2_zero, so2_one, so2_two,
    )
    return result.reshape(features.shape)


def solution(mesh):
    boxes = ("gx", "gy", "gz")
    placed = (
        P(*boxes, None, None), P(*boxes), P(*boxes), P(*boxes, None), P(*boxes, None),
        P(*boxes, None, None), P(*boxes, None, None), P(), P(), P(),
    )
    return jax.shard_map(
        body, mesh=mesh, in_specs=placed, out_specs=P(*boxes, None, None), check_vma=False
    )
```

```python
import jax
import jax.numpy as jnp
from jax import lax
from jax.experimental import pallas as pl
from jax.experimental.pallas import tpu as pltpu
from jax.sharding import PartitionSpec as P

MESH = pl.DeviceIdType.MESH
DEGREE = 4
ORDER = 2
C = 128
A = 16
COEFS = 25
F = COEFS * C
F32 = jnp.float32
BF16 = jnp.bfloat16
NT = (((1,), (1,)), ((), ()))
TN = (((0,), (0,)), ((), ()))

WIG = {}
_at = 0
for _l in range(DEGREE + 1):
    for _m in range(-min(_l, ORDER), min(_l, ORDER) + 1):
        WIG[_l, _m] = _at
        _at += 2 * _l + 1
ROWS = _at

CHUNKS = (((4,), 16, 9), ((3,), 9, 7), ((0, 1, 2), 0, 9))
NCH = len(CHUNKS)
HALVES = ((0, 13 * C), (13 * C, 12 * C))
OWN = 4
XLOW, XHIGH = 9, 10


def kernel(
    feat_h, atoms_h, count_h, et_h, ep_h, wig_h, rad_h, w0_h, w1_h, w2_h,
    out,
    x, et, ep, wig, rad, w0, w1, w2, wb, gate, w0t, w1t, w2t, pick_t, pick_p,
    g, l0, l1, l2, y0, y1, y2, msg,
    sp, sc, ry, sz, rz, st, tc, rt,
    atoms_s, count_s, local, fs, fr, bs, br,
):
    E = et.shape[1]
    gx, gy, gz = lax.axis_index("gx"), lax.axis_index("gy"), lax.axis_index("gz")
    nx, ny, nz = lax.axis_size("gx"), lax.axis_size("gy"), lax.axis_size("gz")
    up = {"gx": lax.rem(gx + 1, nx), "gy": lax.rem(gy + 1, ny), "gz": lax.rem(gz + 1, nz)}
    down = {
        "gx": lax.rem(gx + nx - 1, nx),
        "gy": lax.rem(gy + ny - 1, ny),
        "gz": lax.rem(gz + nz - 1, nz),
    }

    def remote(src, dst, send, recv, axis, where):
        return pltpu.make_async_remote_copy(
            src_ref=src, dst_ref=dst, send_sem=send, recv_sem=recv,
            device_id={axis: where[axis]}, device_id_type=MESH,
        )

    loads = [
        pltpu.make_async_copy(src, dst, local.at[i])
        for i, (src, dst) in enumerate(
            (
                (feat_h, x.at[OWN]), (wig_h, wig), (et_h, et), (ep_h, ep), (rad_h, rad),
                (w0_h, w0), (w1_h, w1), (w2_h, w2), (atoms_h, atoms_s), (count_h, count_s),
            )
        )
    ]
    barrier = pltpu.get_barrier_semaphore()
    for axis in ("gx", "gy", "gz"):
        for where in (up, down):
            pl.semaphore_signal(
                barrier, inc=1, device_id={axis: where[axis]}, device_id_type=MESH
            )
    for load in loads:
        load.start()
    loads[0].wait()
    pl.semaphore_wait(barrier, 6)

    def forward(k, src, dst, axis, where, half=None):
        if half is None:
            return remote(x.at[src], x.at[dst], fs.at[k], fr.at[k], axis, where)
        cols = pl.ds(*HALVES[half])
        k = k + 10 * half
        return remote(x.at[src, :, cols], x.at[dst, :, cols], fs.at[k], fr.at[k], axis, where)

    first = [
        [
            forward(0, OWN, 3, "gz", up, h), forward(1, OWN, 5, "gz", down, h),
            forward(2, OWN, 1, "gy", up, h), forward(3, OWN, 7, "gy", down, h),
        ]
        for h in range(2)
    ]
    towers = [forward(4, OWN, XLOW, "gx", up), forward(5, OWN, XHIGH, "gx", down)]
    relays = [
        [
            forward(6, 3, 0, "gy", up, h), forward(7, 5, 8, "gy", down, h),
            forward(9, 1, 2, "gz", down, h), forward(8, 7, 6, "gz", up, h),
        ]
        for h in range(2)
    ]
    for copy in towers + first[0] + first[1]:
        copy.start()

    def pass_on(half):
        for i in (2, 3, 0, 1):
            first[half][i].wait_recv()
            relays[half][i].start()

    for load in loads[1:]:
        load.wait()
    for o in range(ROWS):
        wb[o] = jnp.broadcast_to(wig[o].astype(BF16), (16, wig.shape[2]))
    gate[...] = rad[...].T
    live = lax.broadcasted_iota(jnp.int32, et.shape, 1) < count_s[0, 0]
    edges = et.shape[1]
    here_t = jnp.where(live, et[...], -1)
    here_p = jnp.where(live, ep[...], -1)
    pick_t[...] = (
        lax.broadcasted_iota(jnp.int32, (3 * A, edges), 0) == here_t
    ).astype(F32).astype(BF16)
    pick_p[...] = (
        lax.broadcasted_iota(jnp.int32, (9 * A, edges), 0) == here_p
    ).astype(F32).astype(BF16)

    def column(i):
        return pl.ds(pl.multiple_of(i * C, C), C)

    def turn0(i, c):
        for k in range(5):
            w0t[k, column(i), :] = w0[k * C : (k + 1) * C, column(i)].T
        return c

    def turn1(i, c):
        for k in range(4):
            w1t[k, column(i), :] = w1[1, k * C : (k + 1) * C, column(i)].T
            w1t[4 + k, column(i), :] = w1[0, k * C : (k + 1) * C, column(i)].T
        return c

    def turn2(i, c):
        for k in range(3):
            w2t[k, column(i), :] = w2[1, k * C : (k + 1) * C, column(i)].T
            w2t[3 + k, column(i), :] = w2[0, k * C : (k + 1) * C, column(i)].T
        return c

    lax.fori_loop(0, 5, turn0, 0)
    lax.fori_loop(0, 4, turn1, 0)
    lax.fori_loop(0, 3, turn2, 0)

    def spread(o):
        return wb[o]

    def added(terms):
        while len(terms) > 1:
            pairs = [a + b for a, b in zip(terms[::2], terms[1::2])]
            terms = pairs + terms[len(terms) - len(terms) % 2 :]
        return terms[0]

    def gather_tower(i, c):
        col = column(i)
        block = jnp.concatenate([x[XLOW, :, col], x[OWN, :, col], x[XHIGH, :, col]], axis=0)
        g[i] = lax.dot_general(block, pick_t[...], TN, preferred_element_type=F32).astype(BF16)
        return c

    def gather_plate(i, c):
        block = x[0:9, :, column(i)].reshape(9 * A, C)
        g[i] = lax.dot_general(block, pick_p[...], TN, preferred_element_type=F32).astype(BF16)
        return c

    def rotate(t, c):
        base = pl.multiple_of(t * 16, 16)
        tile = pl.ds(base, 16)
        scale = gate[tile, :]
        for l in range(DEGREE + 1):
            xs = [g[l * l + j, tile, :] for j in range(2 * l + 1)]
            for m in range(-min(l, ORDER), min(l, ORDER) + 1):
                low = added([spread(WIG[l, m] + j) * xs[j] for j in range(2 * l + 1)]) * scale
                if m == 0:
                    l0[pl.ds(base + l * C, 16), :] = low
                else:
                    ref, size = (l1, 4 * C) if abs(m) == 1 else (l2, 3 * C)
                    at = base + (l - abs(m)) * C
                    if m > 0:
                        ref[pl.ds(at + size, 16), 0:E] = low
                        ref[pl.ds(at, 16), E : 2 * E] = low
                    else:
                        ref[pl.ds(at, 16), 0:E] = -low
                        ref[pl.ds(at + size, 16), E : 2 * E] = low
        return c

    def mix():
        for y, w, low in ((y0, w0t, l0), (y1, w1t, l1), (y2, w2t, l2)):
            table = jnp.concatenate([w[k] for k in range(w.shape[0])], axis=1)
            y[...] = jnp.dot(table, low[...], preferred_element_type=F32).astype(BF16)

    def rotate_back(degrees):
        def step(t, c):
            base = pl.multiple_of(t * 16, 16)
            for l in degrees:
                within = min(l, ORDER)
                ys = {}
                for m in range(-within, within + 1):
                    if m == 0:
                        ys[m] = y0[pl.ds(base + l * C, 16), :]
                    else:
                        ref = y1 if abs(m) == 1 else y2
                        lanes = slice(0, E) if m > 0 else slice(E, 2 * E)
                        ys[m] = ref[pl.ds(base + (l - abs(m)) * C, 16), lanes]
                for j in range(2 * l + 1):
                    msg[l * l + j, pl.ds(base, 16), :] = added(
                        [spread(WIG[l, m] + j) * ys[m] for m in range(-within, within + 1)]
                    )
            return c

        lax.fori_loop(0, 8, step, 0)

    def chunk_cols(q):
        return pl.ds(CHUNKS[q][1] * C, CHUNKS[q][2] * C)

    def back(q, part, i, axis, where):
        cols = chunk_cols(q)
        src, dst = ((sp, ry), (sz, rz), (st, rt))[part]
        k = q * 10 + part * 4 + i
        return remote(
            src.at[i, :, cols], dst.at[i, :, cols], bs.at[k], br.at[k], axis, where
        )

    routes = (
        (("gy", down), ("gz", up), ("gz", down), ("gy", up)),
        (("gy", down), ("gz", down), ("gz", up), ("gy", up)),
        (("gx", down), ("gx", up)),
    )
    backs = [
        [[back(q, part, i, *route) for i, route in enumerate(routes[part])] for part in range(3)]
        for q in range(NCH)
    ]

    def along(q):
        cols = chunk_cols(q)
        for side, corner in ((1, 0), (0, 1), (3, 2), (2, 3)):
            backs[q][0][corner].wait_recv()
            sz[side, :, cols] = (sc[side, :, cols] + ry[corner, :, cols].astype(F32)).astype(BF16)
            backs[q][1][side].start()

    pass_on(0)
    for copy in towers:
        copy.wait_recv()
    lax.fori_loop(0, COEFS, gather_tower, 0, unroll=True)
    pass_on(1)
    lax.fori_loop(0, 8, rotate, 0)
    mix()
    for q, (degrees, low, many) in enumerate(CHUNKS):
        rotate_back(degrees)

        for i in range(low, low + many):
            s = lax.dot_general(pick_p[...], msg[i], NT, preferred_element_type=F32)
            col = pl.ds(i * C, C)
            for k, p in enumerate((0, 2, 6, 8)):
                sp[k, :, col] = s[p * A : (p + 1) * A].astype(BF16)
            for k, p in enumerate((1, 3, 5, 7, 4)):
                sc[k, :, col] = s[p * A : (p + 1) * A]
        for copy in backs[q][0]:
            copy.start()

    for copy in relays[0] + relays[1]:
        copy.wait_recv()
    lax.fori_loop(0, COEFS, gather_plate, 0, unroll=True)
    lax.fori_loop(0, 8, rotate, 0)
    along(0)
    mix()
    along(1)
    for q, (degrees, low, many) in enumerate(CHUNKS):
        rotate_back(degrees)

        for i in range(low, low + many):
            s = lax.dot_general(pick_t[...], msg[i], NT, preferred_element_type=F32)
            col = pl.ds(i * C, C)
            st[0, :, col] = s[0:A].astype(BF16)
            tc[:, col] = s[A : 2 * A]
            st[1, :, col] = s[2 * A : 3 * A].astype(BF16)
        for copy in backs[q][2]:
            copy.start()
        if q == 0:
            along(2)

    for q in range(NCH):
        for copy in backs[q][1] + backs[q][2]:
            copy.wait_recv()

        cols = chunk_cols(q)
        present = lax.broadcasted_iota(jnp.int32, (A, CHUNKS[q][2] * C), 0) < atoms_s[0, 0]
        total = tc[:, cols] + sc[4, :, cols] + x[OWN, :, cols].astype(F32)
        for ref, parts in ((rt, 2), (rz, 4)):
            for i in range(parts):
                total = total + ref[i, :, cols].astype(F32)
        out[:, cols] = jnp.where(present, total, 0.0).astype(BF16)
    for copy in first[0] + first[1] + towers + relays[0] + relays[1]:
        copy.wait_send()
    for q in range(NCH):
        for part in backs[q]:
            for copy in part:
                copy.wait_send()


def body(features, box_atoms, edge_count, edge_tower, edge_plate, wigner, radial, so2_zero, so2_one, so2_two):
    E = edge_tower.shape[3]
    hbm = pl.BlockSpec(memory_space=pl.ANY)
    V = pltpu.VMEM
    dma = pltpu.SemaphoreType.DMA
    result = pl.pallas_call(
        kernel,
        out_shape=jax.ShapeDtypeStruct((A, F), BF16),
        in_specs=[hbm] * 10,
        out_specs=pl.BlockSpec(memory_space=pltpu.VMEM),
        scratch_shapes=[
            V((11, A, F), BF16), V((1, E), jnp.int32), V((1, E), jnp.int32), V((ROWS, 1, E), F32),
            V((E, C), BF16), V((640, 640), BF16), V((2, 512, 512), BF16), V((2, 384, 384), BF16),
            V((ROWS, 16, E), BF16), V((C, E), BF16),
            V((5, 640, C), BF16), V((8, 512, C), BF16), V((6, 384, C), BF16),
            V((3 * A, E), BF16), V((9 * A, E), BF16),
            V((COEFS, C, E), BF16), V((640, E), BF16), V((1024, 2 * E), BF16), V((768, 2 * E), BF16),
            V((640, E), BF16), V((512, 2 * E), BF16), V((384, 2 * E), BF16), V((COEFS, C, E), BF16),
            V((4, A, F), BF16), V((5, A, F), F32), V((4, A, F), BF16),
            V((4, A, F), BF16), V((4, A, F), BF16),
            V((2, A, F), BF16), V((A, F), F32), V((2, A, F), BF16),
            pltpu.SMEM((1, 1), jnp.int32), pltpu.SMEM((1, 1), jnp.int32), dma((10,)), dma((20,)), dma((20,)), dma((10 * NCH,)), dma((10 * NCH,)),
        ],
        compiler_params=pltpu.CompilerParams(
            collective_id=0, has_side_effects=True
        ),
        name="layer",
    )(
        features.reshape(A, F), box_atoms.reshape(1, 1), edge_count.reshape(1, 1),
        edge_tower.reshape(1, E), edge_plate.reshape(1, E),
        wigner.reshape(ROWS, 1, E), radial.reshape(E, C), so2_zero, so2_one, so2_two,
    )
    return result.reshape(features.shape)


def solution(mesh):
    boxes = ("gx", "gy", "gz")
    placed = (
        P(*boxes, None, None), P(*boxes), P(*boxes), P(*boxes, None), P(*boxes, None),
        P(*boxes, None, None), P(*boxes, None, None), P(), P(), P(),
    )
    return jax.shard_map(
        body, mesh=mesh, in_specs=placed, out_specs=P(*boxes, None, None), check_vma=False
    )
```

```python
import jax
import jax.numpy as jnp
from jax import lax
from jax.experimental import pallas as pl
from jax.experimental.pallas import tpu as pltpu
from jax.sharding import PartitionSpec as P

MESH = pl.DeviceIdType.MESH
DEGREE = 4
ORDER = 2
C = 128
A = 16
COEFS = 25
F = COEFS * C
F32 = jnp.float32
BF16 = jnp.bfloat16
NT = (((1,), (1,)), ((), ()))
TN = (((0,), (0,)), ((), ()))

WIG = {}
_at = 0
for _l in range(DEGREE + 1):
    for _m in range(-min(_l, ORDER), min(_l, ORDER) + 1):
        WIG[_l, _m] = _at
        _at += 2 * _l + 1
ROWS = _at

CHUNKS = (((4,), 16, 9), ((3,), 9, 7), ((0, 1, 2), 0, 9))
NCH = len(CHUNKS)
HALVES = ((0, 13 * C), (13 * C, 12 * C))
OWN = 4
XLOW, XHIGH = 9, 10


def kernel(
    feat_h, atoms_h, count_h, et_h, ep_h, wig_h, rad_h, w0_h, w1_h, w2_h,
    out,
    x, et, ep, wig, rad, w0, w1, w2, wb, wf, gate, w0t, w1t, w2t, pick_t, pick_p,
    g, l0, l1, l2, y0, y1, y2, msg,
    sp, sc, ry, sz, rz, st, tc, rt,
    atoms_s, count_s, local, fs, fr, bs, br,
):
    E = et.shape[1]
    gx, gy, gz = lax.axis_index("gx"), lax.axis_index("gy"), lax.axis_index("gz")
    nx, ny, nz = lax.axis_size("gx"), lax.axis_size("gy"), lax.axis_size("gz")
    up = {"gx": lax.rem(gx + 1, nx), "gy": lax.rem(gy + 1, ny), "gz": lax.rem(gz + 1, nz)}
    down = {
        "gx": lax.rem(gx + nx - 1, nx),
        "gy": lax.rem(gy + ny - 1, ny),
        "gz": lax.rem(gz + nz - 1, nz),
    }

    def remote(src, dst, send, recv, axis, where):
        return pltpu.make_async_remote_copy(
            src_ref=src, dst_ref=dst, send_sem=send, recv_sem=recv,
            device_id={axis: where[axis]}, device_id_type=MESH,
        )

    loads = [
        pltpu.make_async_copy(src, dst, local.at[i])
        for i, (src, dst) in enumerate(
            (
                (feat_h, x.at[OWN]), (wig_h, wig), (et_h, et), (ep_h, ep), (rad_h, rad),
                (w0_h, w0), (w1_h, w1), (w2_h, w2), (atoms_h, atoms_s), (count_h, count_s),
            )
        )
    ]
    barrier = pltpu.get_barrier_semaphore()
    for axis in ("gx", "gy", "gz"):
        for where in (up, down):
            pl.semaphore_signal(
                barrier, inc=1, device_id={axis: where[axis]}, device_id_type=MESH
            )
    for load in loads:
        load.start()
    loads[0].wait()
    pl.semaphore_wait(barrier, 6)

    def forward(k, src, dst, axis, where, half=None):
        if half is None:
            return remote(x.at[src], x.at[dst], fs.at[k], fr.at[k], axis, where)
        cols = pl.ds(*HALVES[half])
        k = k + 10 * half
        return remote(x.at[src, :, cols], x.at[dst, :, cols], fs.at[k], fr.at[k], axis, where)

    first = [
        [
            forward(0, OWN, 3, "gz", up, h), forward(1, OWN, 5, "gz", down, h),
            forward(2, OWN, 1, "gy", up, h), forward(3, OWN, 7, "gy", down, h),
        ]
        for h in range(2)
    ]
    towers = [forward(4, OWN, XLOW, "gx", up), forward(5, OWN, XHIGH, "gx", down)]
    relays = [
        [
            forward(6, 3, 0, "gy", up, h), forward(7, 5, 8, "gy", down, h),
            forward(9, 1, 2, "gz", down, h), forward(8, 7, 6, "gz", up, h),
        ]
        for h in range(2)
    ]
    for copy in towers + first[0] + first[1]:
        copy.start()

    def pass_on(half):
        for i in (2, 3, 0, 1):
            first[half][i].wait_recv()
            relays[half][i].start()

    for load in loads[1:]:
        load.wait()
    for o in range(ROWS):
        wf[o] = jnp.broadcast_to(wig[o], (8, wig.shape[2]))
        wb[o] = jnp.broadcast_to(wig[o].astype(BF16), (16, wig.shape[2]))
    gate[...] = rad[...].T
    live = lax.broadcasted_iota(jnp.int32, et.shape, 1) < count_s[0, 0]
    edges = et.shape[1]
    here_t = jnp.where(live, et[...], -1)
    here_p = jnp.where(live, ep[...], -1)
    pick_t[...] = (
        lax.broadcasted_iota(jnp.int32, (3 * A, edges), 0) == here_t
    ).astype(F32).astype(BF16)
    pick_p[...] = (
        lax.broadcasted_iota(jnp.int32, (9 * A, edges), 0) == here_p
    ).astype(F32).astype(BF16)

    def column(i):
        return pl.ds(pl.multiple_of(i * C, C), C)

    def turn0(i, c):
        for k in range(5):
            w0t[k, column(i), :] = w0[k * C : (k + 1) * C, column(i)].T
        return c

    def turn1(i, c):
        for k in range(4):
            w1t[k, column(i), :] = w1[1, k * C : (k + 1) * C, column(i)].T
            w1t[4 + k, column(i), :] = w1[0, k * C : (k + 1) * C, column(i)].T
        return c

    def turn2(i, c):
        for k in range(3):
            w2t[k, column(i), :] = w2[1, k * C : (k + 1) * C, column(i)].T
            w2t[3 + k, column(i), :] = w2[0, k * C : (k + 1) * C, column(i)].T
        return c

    lax.fori_loop(0, 5, turn0, 0)
    lax.fori_loop(0, 4, turn1, 0)
    lax.fori_loop(0, 3, turn2, 0)

    def spread(o):
        return wb[o]

    def spread_full(o):
        row = wf[o]
        return jnp.concatenate([row, row], axis=0)

    def added(terms):
        while len(terms) > 1:
            pairs = [a + b for a, b in zip(terms[::2], terms[1::2])]
            terms = pairs + terms[len(terms) - len(terms) % 2 :]
        return terms[0]

    def gather_tower(i, c):
        col = column(i)
        block = jnp.concatenate([x[XLOW, :, col], x[OWN, :, col], x[XHIGH, :, col]], axis=0)
        g[i] = lax.dot_general(block, pick_t[...], TN, preferred_element_type=F32).astype(BF16)
        return c

    def gather_plate(i, c):
        block = x[0:9, :, column(i)].reshape(9 * A, C)
        g[i] = lax.dot_general(block, pick_p[...], TN, preferred_element_type=F32).astype(BF16)
        return c

    def rotate(t, c):
        base = pl.multiple_of(t * 16, 16)
        tile = pl.ds(base, 16)
        scale = gate[tile, :]
        for l in range(DEGREE + 1):
            xs = [g[l * l + j, tile, :] for j in range(2 * l + 1)]
            for m in range(-min(l, ORDER), min(l, ORDER) + 1):
                low = added([spread(WIG[l, m] + j) * xs[j] for j in range(2 * l + 1)]) * scale
                if m == 0:
                    l0[pl.ds(base + l * C, 16), :] = low
                else:
                    ref, size = (l1, 4 * C) if abs(m) == 1 else (l2, 3 * C)
                    at = base + (l - abs(m)) * C
                    if m > 0:
                        ref[pl.ds(at + size, 16), 0:E] = low
                        ref[pl.ds(at, 16), E : 2 * E] = low
                    else:
                        ref[pl.ds(at, 16), 0:E] = -low
                        ref[pl.ds(at + size, 16), E : 2 * E] = low
        return c

    def mix():
        for y, w, low in ((y0, w0t, l0), (y1, w1t, l1), (y2, w2t, l2)):
            table = jnp.concatenate([w[k] for k in range(w.shape[0])], axis=1)
            y[...] = jnp.dot(table, low[...], preferred_element_type=F32)

    def rotate_back(degrees):
        def step(t, c):
            base = pl.multiple_of(t * 16, 16)
            for l in degrees:
                within = min(l, ORDER)
                ys = {}
                for m in range(-within, within + 1):
                    if m == 0:
                        ys[m] = y0[pl.ds(base + l * C, 16), :]
                    else:
                        ref = y1 if abs(m) == 1 else y2
                        lanes = slice(0, E) if m > 0 else slice(E, 2 * E)
                        ys[m] = ref[pl.ds(base + (l - abs(m)) * C, 16), lanes]
                for j in range(2 * l + 1):
                    msg[l * l + j, pl.ds(base, 16), :] = added(
                        [spread_full(WIG[l, m] + j) * ys[m] for m in range(-within, within + 1)]
                    ).astype(BF16)
            return c

        lax.fori_loop(0, 8, step, 0)

    def chunk_cols(q):
        return pl.ds(CHUNKS[q][1] * C, CHUNKS[q][2] * C)

    def back(q, part, i, axis, where):
        cols = chunk_cols(q)
        src, dst = ((sp, ry), (sz, rz), (st, rt))[part]
        k = q * 10 + part * 4 + i
        return remote(
            src.at[i, :, cols], dst.at[i, :, cols], bs.at[k], br.at[k], axis, where
        )

    routes = (
        (("gy", down), ("gz", up), ("gz", down), ("gy", up)),
        (("gy", down), ("gz", down), ("gz", up), ("gy", up)),
        (("gx", down), ("gx", up)),
    )
    backs = [
        [[back(q, part, i, *route) for i, route in enumerate(routes[part])] for part in range(3)]
        for q in range(NCH)
    ]

    def along(q):
        cols = chunk_cols(q)
        for side, corner in ((1, 0), (0, 1), (3, 2), (2, 3)):
            backs[q][0][corner].wait_recv()
            sz[side, :, cols] = (sc[side, :, cols] + ry[corner, :, cols].astype(F32)).astype(BF16)
            backs[q][1][side].start()

    pass_on(0)
    for copy in towers:
        copy.wait_recv()
    lax.fori_loop(0, COEFS, gather_tower, 0, unroll=True)
    pass_on(1)
    lax.fori_loop(0, 8, rotate, 0)
    mix()
    for q, (degrees, low, many) in enumerate(CHUNKS):
        rotate_back(degrees)

        for i in range(low, low + many):
            s = lax.dot_general(pick_p[...], msg[i], NT, preferred_element_type=F32)
            col = pl.ds(i * C, C)
            for k, p in enumerate((0, 2, 6, 8)):
                sp[k, :, col] = s[p * A : (p + 1) * A].astype(BF16)
            for k, p in enumerate((1, 3, 5, 7, 4)):
                sc[k, :, col] = s[p * A : (p + 1) * A]
        for copy in backs[q][0]:
            copy.start()

    for copy in relays[0] + relays[1]:
        copy.wait_recv()
    lax.fori_loop(0, COEFS, gather_plate, 0, unroll=True)
    lax.fori_loop(0, 8, rotate, 0)
    along(0)
    mix()
    along(1)
    for q, (degrees, low, many) in enumerate(CHUNKS):
        rotate_back(degrees)

        for i in range(low, low + many):
            s = lax.dot_general(pick_t[...], msg[i], NT, preferred_element_type=F32)
            col = pl.ds(i * C, C)
            st[0, :, col] = s[0:A].astype(BF16)
            tc[:, col] = s[A : 2 * A]
            st[1, :, col] = s[2 * A : 3 * A].astype(BF16)
        for copy in backs[q][2]:
            copy.start()
        if q == 0:
            along(2)

    for q in range(NCH):
        for copy in backs[q][1] + backs[q][2]:
            copy.wait_recv()

        cols = chunk_cols(q)
        present = lax.broadcasted_iota(jnp.int32, (A, CHUNKS[q][2] * C), 0) < atoms_s[0, 0]
        total = tc[:, cols] + sc[4, :, cols] + x[OWN, :, cols].astype(F32)
        for ref, parts in ((rt, 2), (rz, 4)):
            for i in range(parts):
                total = total + ref[i, :, cols].astype(F32)
        out[:, cols] = jnp.where(present, total, 0.0).astype(BF16)
    for copy in first[0] + first[1] + towers + relays[0] + relays[1]:
        copy.wait_send()
    for q in range(NCH):
        for part in backs[q]:
            for copy in part:
                copy.wait_send()


def body(features, box_atoms, edge_count, edge_tower, edge_plate, wigner, radial, so2_zero, so2_one, so2_two):
    E = edge_tower.shape[3]
    hbm = pl.BlockSpec(memory_space=pl.ANY)
    V = pltpu.VMEM
    dma = pltpu.SemaphoreType.DMA
    result = pl.pallas_call(
        kernel,
        out_shape=jax.ShapeDtypeStruct((A, F), BF16),
        in_specs=[hbm] * 10,
        out_specs=pl.BlockSpec(memory_space=pltpu.VMEM),
        scratch_shapes=[
            V((11, A, F), BF16), V((1, E), jnp.int32), V((1, E), jnp.int32), V((ROWS, 1, E), F32),
            V((E, C), BF16), V((640, 640), BF16), V((2, 512, 512), BF16), V((2, 384, 384), BF16),
            V((ROWS, 16, E), BF16), V((ROWS, 8, E), F32), V((C, E), BF16),
            V((5, 640, C), BF16), V((8, 512, C), BF16), V((6, 384, C), BF16),
            V((3 * A, E), BF16), V((9 * A, E), BF16),
            V((COEFS, C, E), BF16), V((640, E), BF16), V((1024, 2 * E), BF16), V((768, 2 * E), BF16),
            V((640, E), F32), V((512, 2 * E), F32), V((384, 2 * E), F32), V((COEFS, C, E), BF16),
            V((4, A, F), BF16), V((5, A, F), F32), V((4, A, F), BF16),
            V((4, A, F), BF16), V((4, A, F), BF16),
            V((2, A, F), BF16), V((A, F), F32), V((2, A, F), BF16),
            pltpu.SMEM((1, 1), jnp.int32), pltpu.SMEM((1, 1), jnp.int32), dma((10,)), dma((20,)), dma((20,)), dma((10 * NCH,)), dma((10 * NCH,)),
        ],
        compiler_params=pltpu.CompilerParams(
            collective_id=0, has_side_effects=True
        ),
        name="layer",
    )(
        features.reshape(A, F), box_atoms.reshape(1, 1), edge_count.reshape(1, 1),
        edge_tower.reshape(1, E), edge_plate.reshape(1, E),
        wigner.reshape(ROWS, 1, E), radial.reshape(E, C), so2_zero, so2_one, so2_two,
    )
    return result.reshape(features.shape)


def solution(mesh):
    boxes = ("gx", "gy", "gz")
    placed = (
        P(*boxes, None, None), P(*boxes), P(*boxes), P(*boxes, None), P(*boxes, None),
        P(*boxes, None, None), P(*boxes, None, None), P(), P(), P(),
    )
    return jax.shard_map(
        body, mesh=mesh, in_specs=placed, out_specs=P(*boxes, None, None), check_vma=False
    )
```
